32 devices in a mesh: rows: 8 (over z, core), aux: 4 (over y, x).
Axes of the slice: x: 2, y: 2, z: 4, core: 2. Of those that a mesh axis runs over, the one named last changes fastest.
Arguments:
- pair_coeffs: float32 [36000, 8192], P('aux', 'rows'), may hold values from -0.0625 to 0.0625
- pair_gaps: float32 [8192], P('rows'), may hold values from 0.2 to 20
- trial_vectors: float32 [36000, 128], P('aux'), may hold values from -0.03125 to 0.03125
Outputs:
- vectors_out: float32 [36000, 128], P('aux')
- rayleigh: float32 [128, 128], replicated
The draws below stay inside these ranges and needn't reach their ends.
All inputs are finite; a program needn't handle non-finite values.
Results may differ from the reference program's by a relative error of at most 0.00011.
Values sent between devices are 32-bit elements; how exact they have to be, the bound alone decides.
A program may use at most 128 MiB of HBM per device.

```python
import math
import jax
import jax.numpy as jnp
from jax import lax

NAUX = 36000
K = 128
ITERS = 2
PAIRS = 8192


def shard_levels(stream_key, shape, pieces, low, top_value):
    def one(position, shards_of):
        steps = jax.random.uniform(jax.random.fold_in(jax.random.fold_in(stream_key, 6), position), (shards_of,), jnp.float32, low / len(pieces), top_value / len(pieces))
        return jnp.repeat(jnp.exp(steps), shape[position] // shards_of).reshape((-1,) + (1,) * (len(shape) - position - 1))

    factor_of = one(*pieces[0])
    for cut in pieces[1:]:
        factor_of = factor_of * one(*cut)
    return factor_of


def normal_values(own_key, dims, deviation, bound, pieces=(), kind=jnp.bfloat16):
    drawn = deviation * jax.random.normal(own_key, dims, jnp.float32)
    if pieces:
        drawn = drawn * shard_levels(own_key, dims, pieces, -0.22, 0.18)
    return jnp.clip(drawn, -bound, bound).astype(kind)


def setup_inputs(seed: int = 0) -> dict:
    arg_keys = jax.random.split(jax.random.key(seed), 4)
    return {
        "pair_coeffs": normal_values(arg_keys[0], (NAUX, PAIRS), PAIRS ** -0.5, 0.0625, ((0, 4), (1, 8)), jnp.float32),
        "pair_gaps": jnp.clip(jnp.exp(math.log(20.0) - 4.6051702 * jax.random.uniform(arg_keys[1], (PAIRS,), jnp.float32) ** shard_levels(arg_keys[1], (PAIRS,), ((0, 8),), -0.2, 0.2)), 0.2, 20.0),
        "trial_vectors": normal_values(arg_keys[2], (NAUX, K), NAUX ** -0.5, 0.03125, ((0, 4),), jnp.float32),
    }


def project(pair_coeffs, vectors):
    return lax.dot_general(pair_coeffs.astype(jnp.float32), vectors.astype(jnp.float32), (((0,), (0,)), ((), ())), precision=lax.Precision.HIGHEST, preferred_element_type=jnp.float32)

def reference(pair_coeffs, pair_gaps, trial_vectors):
    highest = lax.Precision.HIGHEST
    weights = 4.0 * pair_gaps / (pair_gaps * pair_gaps + 1.0)
    vectors = trial_vectors
    for step in range(ITERS):
        projected = project(pair_coeffs, vectors)
        scaled = weights[:, None] * projected
        applied = jnp.dot(pair_coeffs.astype(jnp.float32), scaled.astype(jnp.float32), precision=highest, preferred_element_type=jnp.float32)
        correlation = jnp.dot(applied.T.astype(jnp.float32), applied.astype(jnp.float32), precision=highest, preferred_element_type=jnp.float32)
        factor = jnp.linalg.cholesky(correlation)
        vectors = jax.scipy.linalg.solve_triangular(factor, applied.T, lower=True).T
    final_proj = project(pair_coeffs, vectors)
    rayleigh = jnp.dot(final_proj.T.astype(jnp.float32), (weights[:, None] * final_proj).astype(jnp.float32), precision=highest, preferred_element_type=jnp.float32)
    return (vectors, rayleigh)
```

```python
import functools

import jax
import jax.numpy as jnp
from jax import lax
from jax.experimental import pallas as pl
from jax.experimental.pallas import tpu as pltpu
from jax.sharding import PartitionSpec as P

ITERS = 2
MESH = pl.DeviceIdType.MESH
F32 = jnp.float32
BF16 = jnp.bfloat16
HIGHEST = lax.Precision.HIGHEST


def split(x):
    hi = x.astype(BF16)
    return hi, (x - hi.astype(F32)).astype(BF16)


def reduce_kernel(axis, n, x_ref, o_ref, got, rs_send, rs_recv, ag_send, ag_recv):
    me = lax.axis_index(axis)
    rows = x_ref.shape[0] // n

    def block(i):
        return pl.ds(pl.multiple_of(i * rows, 8), rows)

    barrier = pltpu.get_barrier_semaphore()
    for d in range(1, n):
        pl.semaphore_signal(barrier, inc=1, device_id={axis: lax.rem(me + d, n)}, device_id_type=MESH)
    pl.semaphore_wait(barrier, n - 1)
    scatter = []
    for d in range(1, n):
        to = lax.rem(me + d, n)
        copy = pltpu.make_async_remote_copy(
            x_ref.at[block(to)], got.at[d - 1], rs_send.at[d - 1], rs_recv.at[d - 1],
            device_id={axis: to}, device_id_type=MESH)
        copy.start()
        scatter.append(copy)
    total = x_ref[block(me), :]
    for d in range(1, n):
        scatter[d - 1].wait_recv()
        total = total + got[d - 1]
    o_ref[block(me), :] = total
    gather = []
    for d in range(1, n):
        copy = pltpu.make_async_remote_copy(
            o_ref.at[block(me)], o_ref.at[block(me)], ag_send.at[d - 1], ag_recv.at[d - 1],
            device_id={axis: lax.rem(me + d, n)}, device_id_type=MESH)
        copy.start()
        gather.append(copy)
    for d in range(1, n):
        frm = lax.rem(me + n - d, n)
        pltpu.make_async_remote_copy(
            o_ref.at[block(frm)], o_ref.at[block(frm)], ag_send.at[d - 1], ag_recv.at[d - 1],
            device_id={axis: lax.rem(me + d, n)}, device_id_type=MESH).wait_recv()
    for d in range(1, n):
        scatter[d - 1].wait_send()
        gather[d - 1].wait_send()


def all_reduce(x, axis, n, collective_id):
    if n == 1:
        return x
    rows, cols = x.shape
    return pl.pallas_call(
        functools.partial(reduce_kernel, axis, n),
        out_shape=jax.ShapeDtypeStruct(x.shape, F32),
        in_specs=[pl.BlockSpec(memory_space=pltpu.VMEM)],
        out_specs=pl.BlockSpec(memory_space=pltpu.VMEM),
        scratch_shapes=[pltpu.VMEM((n - 1, rows // n, cols), F32)] + [pltpu.SemaphoreType.DMA((n - 1,))] * 4,
        compiler_params=pltpu.CompilerParams(collective_id=collective_id, has_side_effects=True),
        name="reduce_" + axis,
    )(x)


def apply_kernel(n, b_ref, tail_ref, s_ref, a_ref, y_ref, c_ref, bbuf, s2, give, own, pair, got, cat,
                 b_sem, pair_send, pair_recv, rs_send, rs_recv, ag_send, ag_recv, fwd_send, fwd_recv):
    h = n // 2
    me = lax.axis_index("rows")
    z, c = me // 2, lax.rem(me, 2)
    blk = a_ref.shape[1]
    extra = tail_ref.shape[0] // n
    main = blk - extra
    k = s_ref.shape[1]
    pairs = s_ref.shape[0]
    tile = 384 if blk % 384 == 0 else 128
    partner = {"rows": z * 2 + 1 - c}

    def chip(d):
        return lax.rem(z + d, h)

    def peer(d):
        return {"rows": chip(d) * 2 + c}

    order = []
    for d in list(range(1, h)) + [0]:
        order.append((1 - c) * h + chip(d))
        order.append(c * h + chip(d))
    order.append(c * h + z)
    order.append((1 - c) * h + z)
    for d in range(1, h):
        order.append(c * h + chip(h - d))
        order.append((1 - c) * h + chip(h - d))

    def fetch(i):
        slot, j = i % 2, order[i]
        return (
            pltpu.make_async_copy(b_ref.at[pl.ds(pl.multiple_of(j * main, 8), main)],
                                  bbuf.at[slot, pl.ds(0, main)], b_sem.at[slot, 0]),
            pltpu.make_async_copy(tail_ref.at[pl.ds(pl.multiple_of(j * extra, 8), extra)],
                                  bbuf.at[slot, pl.ds(main, extra)], b_sem.at[slot, 1]),
        )

    def start(i):
        for copy in fetch(i):
            copy.start()

    def ready(i):
        for copy in fetch(i):
            copy.wait()

    start(0)
    start(1)
    hi, lo = split(s_ref[...])
    s2[:, :k] = hi
    s2[:, k:] = lo

    def multiply(i, dst, slot_of):
        ready(i)

        def step(t, carry):
            at = pl.ds(pl.multiple_of(t * tile, tile), tile)
            bhi, blo = split(bbuf[i % 2, at, :])
            wide = jnp.dot(bhi, s2[...], preferred_element_type=F32)
            low = jnp.dot(blo, s2[:, :k], preferred_element_type=F32)
            dst[slot_of, at, :] = wide[:, :k] + (wide[:, k:] + low)
            return carry

        lax.fori_loop(0, blk // tile, step, 0)
        if i + 2 < len(order):
            start(i + 2)

    barrier = pltpu.get_barrier_semaphore()
    pl.semaphore_signal(barrier, inc=1, device_id=partner, device_id_type=MESH)
    for d in range(1, h):
        pl.semaphore_signal(barrier, inc=1, device_id=peer(d), device_id_type=MESH)
    pl.semaphore_wait(barrier, h)

    def remote(src, dst, send, recv, to):
        return pltpu.make_async_remote_copy(src, dst, send, recv, device_id=to, device_id_type=MESH)

    sends = []
    scatter = {}
    i = 0
    for d in list(range(1, h)) + [0]:
        multiply(i, give, d)
        over = remote(give.at[d], pair.at[d], pair_send.at[d], pair_recv.at[d], partner)
        over.start()
        sends.append(over)
        multiply(i + 1, own, d)
        i += 2
        over.wait_recv()
        own[d] = own[d] + pair[d]
        if d:
            scatter[d] = remote(own.at[d], got.at[d - 1], rs_send.at[d - 1], rs_recv.at[d - 1], peer(d))
            scatter[d].start()
            sends.append(scatter[d])
    mine = c * h + z
    total = own
    for d in range(1, h):
        scatter[d].wait_recv()
        own[0] = own[0] + got[d - 1]
    a_ref[mine] = own[0]
    for d in range(1, h):
        out = remote(own.at[0], a_ref.at[mine], ag_send.at[d - 1], ag_recv.at[d - 1], peer(d))
        out.start()
        sends.append(out)
    first = remote(own.at[0], a_ref.at[mine], fwd_send.at[0], fwd_recv.at[0], partner)
    first.start()
    sends.append(first)

    y_ref[...] = jnp.zeros_like(y_ref)
    c_ref[...] = jnp.zeros_like(c_ref)

    def project(i):
        a = a_ref[order[i]]
        c_ref[...] += lax.dot_general(a, a, (((0,), (0,)), ((), ())), precision=HIGHEST,
                                      preferred_element_type=F32)
        at = a.T
        ahi, alo = split(at)
        cat[:k, :] = ahi
        cat[k:, :] = alo
        ready(i)

        def step(t, carry):
            cols = pl.ds(pl.multiple_of(t * 256, 256), 256)
            bhi, blo = split(bbuf[i % 2, :, cols])
            wide = jnp.dot(cat[...], bhi, preferred_element_type=F32)
            low = jnp.dot(cat[:k, :], blo, preferred_element_type=F32)
            y_ref[:, cols] += wide[:k] + (wide[k:] + low)
            return carry

        lax.fori_loop(0, pairs // 256, step, 0)
        if i + 2 < len(order):
            start(i + 2)

    project(i)
    theirs = (1 - c) * h + z
    remote(a_ref.at[theirs], a_ref.at[theirs], fwd_send.at[0], fwd_recv.at[0], partner).wait_recv()
    project(i + 1)
    i += 2
    for d in range(1, h):
        came = c * h + chip(h - d)
        remote(a_ref.at[came], a_ref.at[came], ag_send.at[d - 1], ag_recv.at[d - 1], peer(d)).wait_recv()
        over = remote(a_ref.at[came], a_ref.at[came], fwd_send.at[d], fwd_recv.at[d], partner)
        over.start()
        sends.append(over)
        project(i)
        came = (1 - c) * h + chip(h - d)
        remote(a_ref.at[came], a_ref.at[came], fwd_send.at[d], fwd_recv.at[d], partner).wait_recv()
        project(i + 1)
        i += 2
    for copy in sends:
        copy.wait_send()


def apply(b, tail, s, n, blk):
    pairs, k = s.shape
    h = n // 2
    dma = pltpu.SemaphoreType.DMA
    vmem = pl.BlockSpec(memory_space=pltpu.VMEM)
    anywhere = pl.BlockSpec(memory_space=pl.ANY)
    return pl.pallas_call(
        functools.partial(apply_kernel, n),
        out_shape=(jax.ShapeDtypeStruct((n, blk, k), F32), jax.ShapeDtypeStruct((k, pairs), F32),
                   jax.ShapeDtypeStruct((k, k), F32)),
        in_specs=[anywhere, anywhere, vmem],
        out_specs=(vmem, vmem, vmem),
        scratch_shapes=[
            pltpu.VMEM((2, blk, pairs), F32),
            pltpu.VMEM((pairs, 2 * k), BF16),
            pltpu.VMEM((h, blk, k), F32),
            pltpu.VMEM((h, blk, k), F32),
            pltpu.VMEM((h, blk, k), F32),
            pltpu.VMEM((h - 1, blk, k), F32),
            pltpu.VMEM((2 * k, blk), BF16),
            dma((2, 2)), dma((h,)), dma((h,)), dma((h - 1,)), dma((h - 1,)),
            dma((h - 1,)), dma((h - 1,)), dma((h,)), dma((h,)),
        ],
        compiler_params=pltpu.CompilerParams(collective_id=0, has_side_effects=True,
                                             vmem_limit_bytes=56 * 1024 * 1024),
        name="apply",
    )(b, tail, s)


def solution(mesh):
    n = mesh.shape["rows"]
    aux = mesh.shape["aux"]

    def shards(b, gaps, trial):
        rows, k = trial.shape
        main = rows // (16 * n) * 16
        blk = (main + 16 + 127) // 128 * 128
        extra = blk - main
        left = rows - n * main
        tail = jnp.pad(b[n * main:], ((0, n * extra - left), (0, 0)))
        weights = (4.0 * gaps / (gaps * gaps + 1.0))[None, :]
        yt = lax.dot_general(trial, b, (((0,), (0,)), ((), ())), precision=lax.Precision.HIGH,
                             preferred_element_type=F32)
        pt = all_reduce(yt, "aux", aux, 1)
        for step in range(ITERS):
            a, yt, gram = apply(b, tail, (pt * weights).T, n, blk)
            both = all_reduce(jnp.concatenate([yt, gram], axis=1), "aux", aux, 2)
            factor = jnp.linalg.cholesky(both[:, -k:])
            inverse = jax.scipy.linalg.solve_triangular(factor, jnp.eye(k, dtype=F32), lower=True)
            pt = jnp.dot(inverse, both[:, :-k], precision=HIGHEST, preferred_element_type=F32)
        v = lax.dot_general(a, inverse, (((2,), (1,)), ((), ())), precision=lax.Precision.HIGH,
                            preferred_element_type=F32)
        vectors = jnp.concatenate([v[:, :main].reshape(n * main, k), v[:, main:].reshape(n * extra, k)[:left]])
        part = lax.dot_general(pt, pt * weights, (((1,), (1,)), ((), ())), precision=HIGHEST,
                               preferred_element_type=F32)
        return vectors, all_reduce(part, "rows", n, 3)

    in_specs = (P("aux", "rows"), P("rows"), P("aux", None))
    return jax.shard_map(shards, mesh=mesh, in_specs=in_specs, out_specs=(P("aux", None), P()), check_vma=False)
```
